8 devices in a mesh: data: 8 (over z, y, x, core).
Axes of the slice: x: 2, y: 2, z: 1, core: 2. Of those that a mesh axis runs over, the one named last changes fastest.
Arguments:
- x_in: bfloat16 [32768, 1024], P('data')
- dy_in: bfloat16 [32768, 1024], P('data')
- weights: bfloat16 [4, 1024, 1024], replicated
- a_old: float32 [4096, 1024], P('data')
- s_old: float32 [4096, 1024], P('data')
- a_inv: float32 [4096, 1024], P('data')
- s_inv: float32 [4, 1024, 1024], replicated
Outputs:
- output 1: float32 [4, 1024, 1024], replicated
- output 2: float32 [4096, 1024], P('data')
- output 3: float32 [4096, 1024], P('data')
All inputs are finite; a program needn't handle non-finite values.
Results may differ from the reference program's by a relative error of at most 0.001.
Values are sent between devices in bfloat16 or wider.
A program may use at most 1 GiB of HBM per device.

```python
import functools
import jax
import jax.numpy as jnp

D = 1024
LAYERS = 4
TOKENS = 4096
SHARDS = 8
LOW_RANK = 64
BATCH_TOTAL = TOKENS * SHARDS
FACTOR_DECAY = 0.75


def spd_stack(rng_key, base_diag, gram_scale):
    low_rank = jax.random.normal(rng_key, (LAYERS, D, LOW_RANK), jnp.float32)
    gram_mat = jnp.einsum("lir,ljr->lij", low_rank, low_rank)
    gram_mat = 0.5 * (gram_mat + jnp.swapaxes(gram_mat, 1, 2))
    return gram_scale * gram_mat + base_diag * jnp.eye(D, dtype=jnp.float32)


def shard_rows(rng_key, spread):
    key_raw, key_mean, key_scale = jax.random.split(rng_key, 3)
    raw_rows = jax.random.normal(key_raw, (SHARDS, TOKENS, D), jnp.float32)
    offset = 0.7 * jax.random.normal(key_mean, (SHARDS, 1, D), jnp.float32)
    row_scale = jnp.exp(spread * jax.random.normal(key_scale, (SHARDS, 1, 1), jnp.float32))
    return ((raw_rows + offset) * row_scale).reshape(BATCH_TOTAL, D).astype(jnp.bfloat16)


def setup_inputs(seed: int = 0) -> dict:
    key_list = jax.random.split(jax.random.key(seed), 7)
    weights = jax.random.normal(key_list[2], (LAYERS, D, D), jnp.float32) * D ** -0.5
    inv_scale = (LOW_RANK * D) ** -0.5
    return {
        "x_in": shard_rows(key_list[0], 0.5),
        "dy_in": shard_rows(key_list[1], 0.5),
        "weights": weights.astype(jnp.bfloat16),
        "a_old": spd_stack(key_list[3], 0.5, 1.0 / LOW_RANK).reshape(LAYERS * D, D),
        "s_old": spd_stack(key_list[4], 0.5, 1.0 / LOW_RANK).reshape(LAYERS * D, D),
        "a_inv": spd_stack(key_list[5], 0.5, inv_scale).reshape(LAYERS * D, D),
        "s_inv": spd_stack(key_list[6], 0.5, inv_scale),
    }


def gelu_grad(pre_act, d_act):
    pullback = jax.vjp(functools.partial(jax.nn.gelu, approximate=True), pre_act.astype(jnp.float32))[1]
    return pullback(d_act.astype(jnp.float32))[0].astype(jnp.bfloat16)


def reference(x_in, dy_in, weights, a_old, s_old, a_inv, s_inv):
    layer_inputs = [x_in]
    pre_acts = []
    for layer_id in range(LAYERS - 1):
        pre_act = jnp.dot(layer_inputs[layer_id], weights[layer_id], preferred_element_type=jnp.float32).astype(jnp.bfloat16)
        pre_acts.append(pre_act)
        layer_inputs.append(jax.nn.gelu(pre_act.astype(jnp.float32), approximate=True).astype(jnp.bfloat16))
    out_grads = [dy_in] * LAYERS
    for layer_id in range(LAYERS - 1, 0, -1):
        d_act = jnp.dot(out_grads[layer_id], weights[layer_id].T, preferred_element_type=jnp.float32).astype(jnp.bfloat16)
        out_grads[layer_id - 1] = gelu_grad(pre_acts[layer_id - 1], d_act)
    a_facs = []
    s_facs = []
    updates = []
    for layer_id in range(LAYERS):
        h_in = layer_inputs[layer_id]
        g_out = out_grads[layer_id]
        a_facs.append(jnp.dot(h_in.T, h_in, preferred_element_type=jnp.float32) / BATCH_TOTAL)
        s_facs.append(jnp.dot(g_out.T, g_out, preferred_element_type=jnp.float32) / BATCH_TOTAL)
        w_grad = jnp.dot(h_in.T, g_out, preferred_element_type=jnp.float32) / BATCH_TOTAL
        a_inv_layer = a_inv[layer_id * D:(layer_id + 1) * D]
        updates.append(jnp.dot(a_inv_layer, jnp.dot(w_grad, s_inv[layer_id])))
    a_new = FACTOR_DECAY * a_old + (1.0 - FACTOR_DECAY) * jnp.concatenate(a_facs, axis=0)
    s_new = FACTOR_DECAY * s_old + (1.0 - FACTOR_DECAY) * jnp.concatenate(s_facs, axis=0)
    return (jnp.stack(updates), a_new, s_new)
```

```python
import functools
import math
import jax
import jax.numpy as jnp
from jax import lax
from jax.experimental import pallas as pl
from jax.experimental.pallas import tpu as pltpu
from jax.sharding import PartitionSpec as P

F32 = jnp.float32
BF16 = jnp.bfloat16
MESH = pl.DeviceIdType.MESH
PRECISE = lax.Precision.HIGHEST
FACTOR_DECAY = 0.75
GELU_A = math.sqrt(2.0 / math.pi)
GELU_B = GELU_A * 0.044715

D = 1024
BK = 512
HALF = D // 2
PR, PC = 256, 1280


def gelu(z):
    hz = 0.5 * z
    return hz + hz * jnp.tanh(z * (GELU_A + GELU_B * (z * z)))


def gelu_slope(z):
    m = GELU_B * (z * z)
    t = jnp.tanh(z * (GELU_A + m))
    return (0.5 + 0.5 * t) + (0.5 * z) * (1.0 - t * t) * (GELU_A + 3.0 * m)


def rows_dot(a, b):
    return lax.dot_general(a, b, (((0,), (0,)), ((), ())), preferred_element_type=F32)


def add_gram(acc, slot, v):
    c = [slice(256 * j, 256 * (j + 1)) for j in range(4)]
    acc[slot, 0, :, 0:1024] += rows_dot(v[:, c[0]], v)
    acc[slot, 0, :, 1024:1280] += rows_dot(v[:, c[1]], v[:, c[1]])
    acc[slot, 1, :, 0:512] += rows_dot(v[:, c[1]], v[:, 512:])
    acc[slot, 1, :, 512:1024] += rows_dot(v[:, c[2]], v[:, 512:])
    acc[slot, 1, :, 1024:1280] += rows_dot(v[:, c[3]], v[:, c[3]])


class Sems:
    def __init__(self):
        self.n = 0

    def take(self, n=1):
        i = self.n
        self.n += n
        return i


def mega_kernel(nb, x, dy, w, ainv, sinv,
                u, own_a, oth_a, own_s, oth_s, hs, zs, gs, og, oa, os_, qg, qp,
                inb, outb, wb, acc_g, acc_p, d_g, d_p, stage, ain,
                in_sem, out_sem, w_sem, loc_sem, snd, rcv, usnd, urcv):
    dev = lax.axis_index("data")
    k = dev % 2
    c = dev // 2
    cx = c % 2
    cy = c // 2
    partner = 2 * c + (1 - k)
    xn = 2 * (2 * cy + (1 - cx)) + k
    yn = 2 * (2 * (1 - cy) + cx) + k

    def rdma(src, dst, ss, rs, to):
        return pltpu.make_async_remote_copy(src_ref=src, dst_ref=dst, send_sem=ss, recv_sem=rs,
                                            device_id=(to,), device_id_type=MESH)

    def local(src, dst, i):
        return pltpu.make_async_copy(src, dst, loc_sem.at[i])

    class Job:
        def __init__(self, kind, layer, slot):
            self.o = layer
            o = layer
            self.dg = 3 - o
            self.nx = (o // 2) * 2 + (1 - o % 2)
            self.ny = (1 - o // 2) * 2 + o % 2
            if kind == "g":
                self.acc = lambda h: acc_g.at[slot, pl.ds(h * HALF, HALF)]
                self.d, self.q, self.oo = d_g.at[layer], qg.at[layer], og
                self.rows, base = HALF, 24 * 0 + layer
                self.ch = 64
            else:
                self.acc = lambda h: acc_p.at[slot, h]
                i = layer if kind == "a" else 4 + layer
                self.d, self.q, self.oo = d_p.at[i], qp.at[i], (oa if kind == "a" else os_)
                self.rows, base = PR, 4 + i
                self.ch = 32
            self.s0 = 3 * base
            self.r0 = 6 * base
            r2 = self.rows // 2
            self.a, self.b = pl.ds(0, r2), pl.ds(r2, r2)

        def d2d(self):
            return rdma(self.acc(1 - k), self.d, snd.at[self.s0], rcv.at[self.r0], partner)

        def start(self):
            self.d2d().start()

        def finish(self):
            cp = self.d2d()
            cp.wait_recv()

            def add(i, _):
                r = pl.ds(i * self.ch, self.ch)
                self.d[r] = self.d[r] + self.acc(k)[r]
                return 0
            lax.fori_loop(0, self.rows // self.ch, add, 0)
            cp.wait_send()

        def sends(self, role):
            s1, s2 = snd.at[self.s0 + 1], snd.at[self.s0 + 2]
            r = self.r0
            d, q, oo, a, b = self.d, self.q, self.oo, self.a, self.b
            if role == "dg":
                return rdma(d.at[a], q, s1, rcv.at[r + 1], xn), rdma(d.at[b], q, s2, rcv.at[r + 1], yn)
            if role == "nx":
                return (rdma(d.at[a], oo.at[0, a], s1, rcv.at[r + 2], xn),
                        rdma(d.at[b], oo.at[0, b], s2, rcv.at[r + 3], xn))
            return (rdma(d.at[b], oo.at[1, b], s1, rcv.at[r + 4], yn),
                    rdma(d.at[a], oo.at[1, a], s2, rcv.at[r + 5], yn))

        def hop1(self):
            @pl.when(c == self.dg)
            def _():
                one, two = self.sends("dg")
                one.start()
                two.start()

            @pl.when(c == self.nx)
            def _():
                self.sends("nx")[0].start()

            @pl.when(c == self.ny)
            def _():
                self.sends("ny")[0].start()

        def hop2(self):
            r2 = self.rows // 2
            st = stage.at[:, pl.ds(0, D)] if self.rows == HALF else stage.at[pl.ds(0, r2)]

            def go(role, part, off):
                self.sends("dg")[0].wait_recv()
                cp = local(self.q, st, 0)
                cp.start()
                cp.wait()

                def add(i, _):
                    r = pl.ds(off + i * self.ch, self.ch)
                    self.d[r] = self.d[r] + st[pl.ds(i * self.ch, self.ch)]
                    return 0
                lax.fori_loop(0, r2 // self.ch, add, 0)
                self.sends(role)[1].start()

            @pl.when(c == self.nx)
            def _():
                go("nx", self.b, r2)

            @pl.when(c == self.ny)
            def _():
                go("ny", self.a, 0)

        def drain(self):
            for role, chip in (("dg", self.dg), ("nx", self.nx), ("ny", self.ny)):
                @pl.when(c == chip)
                def _():
                    one, two = self.sends(role)
                    one.wait_send()
                    two.wait_send()

        def arrive(self):
            @pl.when(c == self.o)
            def _():
                for role in ("nx", "ny"):
                    one, two = self.sends(role)
                    one.wait_recv()
                    two.wait_recv()

    slots_p = {"a0": 0, "s3": 1, "a1": 2, "a2": 0, "s2": 1, "a3": 2, "s1": 0, "s0": 1}
    job = {f"g{l}": Job("g", l, (3 - l) % 2) for l in range(4)}
    for l in range(4):
        job[f"a{l}"] = Job("a", l, slots_p[f"a{l}"])
        job[f"s{l}"] = Job("s", l, slots_p[f"s{l}"])

    def ev(what, *names):
        return [functools.partial(getattr(Job, what), job[n]) for n in names]

    def load(srcs, i, slot):
        return [pltpu.make_async_copy(s.at[pl.ds(i * BK, BK)], inb.at[j, slot], in_sem.at[j, slot])
                for j, s in enumerate(srcs)]

    def phase(srcs, dsts, body, hooks, zero, nxt, w_next=None):
        def step(i, _):
            slot = i % 2

            @pl.when(i + 1 < nb)
            def _():
                for cp in load(srcs, i + 1, 1 - slot):
                    cp.start()
            if nxt is not None:
                @pl.when(i + 1 == nb)
                def _():
                    for cp in load(nxt, 0, 1 - slot):
                        cp.start()
            for cp in load(srcs, i, slot):
                cp.wait()

            def store(i):
                return [pltpu.make_async_copy(outb.at[j, slot], t.at[pl.ds(i * BK, BK)], out_sem.at[j, slot])
                        for j, t in enumerate(dsts)]
            if dsts:
                @pl.when(i >= 2)
                def _():
                    for cp in store(i - 2):
                        cp.wait()

            @pl.when(i == 0)
            def _():
                for z in zero:
                    z[...] = jnp.zeros(z.shape, F32)
            for at in sorted(hooks):
                @pl.when(i == at)
                def _():
                    for f in hooks[at]:
                        f()
            body([inb.at[j, slot] for j in range(len(srcs))], [outb.at[j, slot] for j in range(len(dsts))])
            for cp in store(i):
                cp.start()
            return 0
        lax.fori_loop(0, nb, step, 0)
        for back in (2, 1):
            for j, t in enumerate(dsts):
                i = nb - back
                pltpu.make_async_copy(outb.at[j, i % 2], t.at[pl.ds(i * BK, BK)], out_sem.at[j, i % 2]).wait()

    def w_copy(l, slot):
        return pltpu.make_async_copy(w.at[l], wb.at[slot], w_sem.at[slot])

    def fwd_body(wslot, pslot, extra=None):
        def body(ins, outs):
            v = ins[0][...]
            z = jnp.dot(v, wb[wslot], preferred_element_type=F32).astype(BF16)
            outs[0][...] = z
            add_gram(acc_p, pslot, v)
            if extra is not None:
                add_gram(acc_p, extra, ins[1][...])
            outs[1][...] = gelu(z.astype(F32)).astype(BF16)
        return body

    def bwd_body(wslot, gslot, pslot=None):
        def body(ins, outs):
            g = ins[0][...]
            d = lax.dot_general(g, wb[wslot], (((1,), (1,)), ((), ())), preferred_element_type=F32).astype(BF16)
            acc_g[gslot] += rows_dot(ins[1][...], g)
            if pslot is not None:
                add_gram(acc_p, pslot, g)
            outs[0][...] = (d.astype(F32) * gelu_slope(ins[2][...].astype(F32))).astype(BF16)
        return body

    def cross_body(gslot):
        def body(ins, outs):
            acc_g[gslot] += rows_dot(ins[1][...], ins[0][...])
        return body

    def gram_body(*pslots):
        def body(ins, outs):
            for j, p in enumerate(pslots):
                add_gram(acc_p, p, ins[j][...])
        return body

    def u_rows(l, q):
        return u.at[l, pl.ds(k * HALF + q * (HALF // 2), HALF // 2)]

    def u_src(l, q):
        return d_g.at[l, pl.ds(q * (HALF // 2), HALF // 2)]

    def owner_sends(l):
        a = [rdma(u_src(l, q), u_rows(l, q), usnd.at[l, q], urcv.at[l, q], xn) for q in (0, 1)]
        b = [rdma(u_src(l, q), u_rows(l, q), usnd.at[l, 2 + q], urcv.at[l, q], yn) for q in (1, 0)]
        p = [rdma(u_src(l, q), u_rows(l, q), usnd.at[l, 4 + q], urcv.at[l, 2 + q], partner) for q in (0, 1)]
        return a + b + p

    def t_copy():
        half = acc_g.at[0, pl.ds(k * HALF, HALF)]
        return rdma(half, half, usnd.at[4, 0], urcv.at[4, 0], partner)

    def u_stage(chips):
        for l in chips:
            job[f"g{l}"].arrive()
        cond = functools.reduce(jnp.logical_or, [c == l for l in chips])

        @pl.when(cond)
        def _():
            cps = [local(ainv, ain, 1)] + [local(og.at[j], acc_g.at[1, pl.ds(j * HALF, HALF)], 2 + j) for j in (0, 1)]
            for cp in cps:
                cp.start()
            for cp in cps:
                cp.wait()

            def add(i, _):
                r, r2 = pl.ds(i * 64, 64), pl.ds(HALF + i * 64, 64)
                d_g[c, r] = d_g[c, r] + (acc_g[1, r] + acc_g[1, r2])
                return 0
            lax.fori_loop(0, HALF // 64, add, 0)
            cp = local(sinv.at[c], acc_g.at[1], 4)
            cp.start()
            cp.wait()
            t = jnp.dot(d_g[c], acc_g[1], precision=PRECISE, preferred_element_type=F32)
            acc_g[0, pl.ds(k * HALF, HALF)] = t * (1.0 / (nb * BK * 8))
            t_copy().start()
            t_copy().wait()
            d_g[c] = jnp.dot(ain[...], acc_g[0], precision=PRECISE, preferred_element_type=F32)
            for s in owner_sends(c):
                s.start()
            local(d_g.at[c], u.at[c, pl.ds(k * HALF, HALF)], 5).start()

    def role_of(o):
        return 3 - o, (o // 2) * 2 + (1 - o % 2), (1 - o // 2) * 2 + o % 2

    def to_partner(o, q):
        return rdma(u_rows(o, q), u_rows(o, q), usnd.at[o, q], urcv.at[o, 2 + q], partner)

    def got(o, q):
        rdma(u_rows(o, q), u_rows(o, q), usnd.at[o, 4], urcv.at[o, q], partner).wait_recv()

    def relay(o, q, to):
        return rdma(u_rows(o, q), u_rows(o, q), usnd.at[o, 4], urcv.at[o, q], to)

    def fan1(o):
        dg, nx, ny = role_of(o)

        @pl.when(c == nx)
        def _():
            got(o, 0)
            relay(o, 0, yn).start()
            to_partner(o, 0).start()

        @pl.when(c == ny)
        def _():
            got(o, 1)
            relay(o, 1, xn).start()
            to_partner(o, 1).start()

    def fan2(o):
        dg, nx, ny = role_of(o)

        @pl.when(c == nx)
        def _():
            got(o, 1)
            to_partner(o, 1).start()

        @pl.when(c == ny)
        def _():
            got(o, 0)
            to_partner(o, 0).start()

        @pl.when(c == dg)
        def _():
            for q in (0, 1):
                got(o, q)
                to_partner(o, q).start()

    def fan3(o):
        dg, nx, ny = role_of(o)

        @pl.when(c == nx)
        def _():
            relay(o, 0, yn).wait_send()

        @pl.when(c == ny)
        def _():
            relay(o, 1, xn).wait_send()

        @pl.when(c != o)
        def _():
            for q in (0, 1):
                to_partner(o, q).wait_send()

        @pl.when(c == o)
        def _():
            for s in owner_sends(o):
                s.wait_send()
            local(d_g.at[o], u.at[o, pl.ds(k * HALF, HALF)], 5).wait()
        for q in (0, 1):
            to_partner(o, q).wait_recv()

    ap = [acc_p.at[i] for i in range(3)]
    ag = [acc_g.at[i] for i in range(2)]
    h = [x, hs.at[0], hs.at[1], hs.at[2]]
    g = [gs.at[0], gs.at[1], gs.at[2], dy]
    s_f1, s_f2, s_f3 = [h[0], dy], [h[1]], [h[2]]
    s_b4, s_b3, s_b2 = [g[3], h[3], zs.at[2]], [g[2], h[2], zs.at[1]], [g[1], h[1], zs.at[0]]
    s_l1 = [g[0], h[0]]
    s_l2, s_l3 = [h[3]], [g[1], g[0]]

    w_copy(0, 0).start()
    for cp in load(s_f1, 0, 0):
        cp.start()
    w_copy(0, 0).wait()
    w_copy(1, 1).start()
    phase(s_f1, [zs.at[0], hs.at[0]], fwd_body(0, 0, 1), {}, [ap[0], ap[1]], s_f2)
    w_copy(1, 1).wait()
    w_copy(2, 0).start()
    phase(s_f2, [zs.at[1], hs.at[1]], fwd_body(1, 2),
          {0: ev("start", "a0", "s3"), 1: ev("finish", "a0", "s3") + ev("hop1", "a0", "s3"),
           6: ev("hop2", "a0", "s3")}, [ap[2]], s_f3)
    w_copy(2, 0).wait()
    w_copy(3, 1).start()
    phase(s_f3, [zs.at[2], hs.at[2]], fwd_body(0, 0),
          {0: ev("start", "a1"), 1: ev("finish", "a1") + ev("hop1", "a1"), 6: ev("hop2", "a1")}, [ap[0]], s_b4)
    w_copy(3, 1).wait()
    w_copy(2, 0).start()
    phase(s_b4, [gs.at[2]], bwd_body(1, 0),
          {0: ev("start", "a2"), 1: ev("finish", "a2") + ev("hop1", "a2"), 5: ev("hop2", "a2")}, [ag[0]], s_b3)
    w_copy(2, 0).wait()
    w_copy(1, 1).start()
    phase(s_b3, [gs.at[1]], bwd_body(0, 1, 1),
          {0: ev("start", "g3"), 1: ev("finish", "g3") + ev("hop1", "g3"),
           7: ev("hop2", "g3")}, [ag[1], ap[1]], s_b2)
    w_copy(1, 1).wait()
    phase(s_b2, [gs.at[0]], bwd_body(1, 0),
          {0: ev("start", "g2", "s2"), 1: ev("finish", "g2", "s2") + ev("hop1", "g2", "s2"),
           7: ev("hop2", "g2", "s2")}, [ag[0]], s_l1)
    phase(s_l1, [], cross_body(1),
          {0: ev("start", "g1"), 2: ev("finish", "g1") + ev("hop1", "g1")}, [ag[1]], s_l2)
    for f in ev("start", "g0") + ev("finish", "g0") + ev("hop1", "g0"):
        f()
    u_stage((3, 2))
    phase(s_l2, [], gram_body(2), {}, [ap[2]], s_l3)
    for f in ev("start", "a3") + ev("hop2", "g1", "g0"):
        f()
    phase(s_l3, [], gram_body(0, 1), {1: ev("finish", "a3") + ev("hop1", "a3")}, [ap[0], ap[1]], None)
    for f in ev("start", "s1", "s0") + ev("finish", "s1", "s0") + ev("hop1", "s1", "s0"):
        f()
    for o in (3, 2):
        fan1(o)
    for f in ev("hop2", "a3"):
        f()
    u_stage((1, 0))
    for f in ev("hop2", "s1", "s0"):
        f()
    for o in (3, 2):
        fan2(o)
    for n in ("a0", "a1", "a2", "a3", "s3", "s2", "s1", "s0", "g3", "g2", "g1", "g0"):
        job[n].drain()
        if n[0] != "g":
            job[n].arrive()

    fin = []
    for j, (src, mine, other) in enumerate(((oa, own_a, oth_a), (os_, own_s, oth_s))):
        local(src, acc_p.at[j], 6 + j).start()
    for j, (src, mine, other) in enumerate(((oa, own_a, oth_a), (os_, own_s, oth_s))):
        local(src, acc_p.at[j], 6 + j).wait()

        def add(i, _):
            r = pl.ds(i * 32, 32)
            d_p[4 * j + c, r] = d_p[4 * j + c, r] + (acc_p[j, 0, r] + acc_p[j, 1, r])
            return 0
        lax.fori_loop(0, PR // 32, add, 0)
        own = d_p.at[4 * j + c]
        fin.append((rdma(own, other, usnd.at[4, 1 + j], urcv.at[4, 1 + j], partner), local(own, mine, 8 + j)))
    for r, cp in fin:
        r.start()
        cp.start()
    for o in (1, 0):
        fan1(o)
    for o in (1, 0):
        fan2(o)
    for o in range(4):
        fan3(o)
    for r, cp in fin:
        r.wait()
        cp.wait()


def mega(x, dy, w, ainv, sinv):
    n = x.shape[0]
    nb = n // BK
    hbm = pl.BlockSpec(memory_space=pltpu.HBM)

    def sh(s, t=F32):
        return jax.ShapeDtypeStruct(s, t)
    half = (PR, PC)
    outs = [sh((4, D, D)), sh(half), sh(half), sh(half), sh(half),
            sh((3, n, D), BF16), sh((3, n, D), BF16), sh((3, n, D), BF16),
            sh((2, HALF, D)), sh((2,) + half), sh((2,) + half), sh((4, HALF // 2, D)), sh((8, PR // 2, PC))]
    dma = pltpu.SemaphoreType.DMA
    return pl.pallas_call(
        functools.partial(mega_kernel, nb),
        out_shape=outs,
        in_specs=[hbm] * 5,
        out_specs=[hbm] * len(outs),
        scratch_shapes=[
            pltpu.VMEM((3, 2, BK, D), BF16), pltpu.VMEM((2, 2, BK, D), BF16), pltpu.VMEM((2, D, D), BF16),
            pltpu.VMEM((2, D, D), F32), pltpu.VMEM((3, 2) + half, F32),
            pltpu.VMEM((4, HALF, D), F32), pltpu.VMEM((8,) + half, F32), pltpu.VMEM((HALF // 2, PC), F32),
            pltpu.VMEM((HALF, D), F32),
            dma((3, 2)), dma((2, 2)), dma((2,)), dma((10,)), dma((36,)), dma((72,)), dma((5, 6)), dma((5, 4)),
        ],
        compiler_params=pltpu.CompilerParams(has_side_effects=True, vmem_limit_bytes=66_000_000),
        name="kfac",
    )(x, dy, w, ainv, sinv)


def finish_kernel(ka, oa, ob, os_, ot, a_old, s_old, a_new, s_new):
    scale = (1.0 - FACTOR_DECAY) / (8 * 4096)

    def blend(old, new, r, cs, v):
        new[r, cs] = FACTOR_DECAY * old[r, cs] + scale * v
    c = [slice(256 * j, 256 * (j + 1)) for j in range(5)]
    for own, oth, old, new in ((oa, ob, a_old, a_new), (os_, ot, s_old, s_new)):
        @pl.when(ka[0] == 0)
        def _():
            blend(old, new, c[0], slice(0, 1024), own[:, 0:1024])
            blend(old, new, c[1], c[0], own[:, c[1]].T)
            blend(old, new, c[1], c[1], own[:, c[4]])
            blend(old, new, c[1], slice(512, 1024), oth[:, 0:512])

        @pl.when(ka[0] == 1)
        def _():
            blend(old, new, c[0], c[0], oth[:, c[2]].T)
            blend(old, new, c[0], c[1], own[:, c[0]].T)
            blend(old, new, c[0], slice(512, 1024), own[:, 512:1024])
            blend(old, new, c[1], c[0], oth[:, c[3]].T)
            blend(old, new, c[1], c[1], own[:, c[1]].T)
            blend(old, new, c[1], c[2], own[:, c[3]].T)
            blend(old, new, c[1], c[3], own[:, c[4]])


def finish(core, oa, ob, os_, ot, a_old, s_old):
    sd = jax.ShapeDtypeStruct((HALF, D), F32)
    return pl.pallas_call(
        finish_kernel,
        out_shape=[sd, sd],
        in_specs=[pl.BlockSpec(memory_space=pltpu.SMEM)] + [pl.BlockSpec(memory_space=pltpu.VMEM)] * 6,
        out_specs=[pl.BlockSpec(memory_space=pltpu.VMEM)] * 2,
        compiler_params=pltpu.CompilerParams(vmem_limit_bytes=40 * 2**20),
        name="blend",
    )(core, oa, ob, os_, ot, a_old, s_old)


def solution(mesh):
    def device_step(x_loc, dy_loc, weights, a_old_rows, s_old_rows, a_inv_rows, s_inv):
        res = mega(x_loc, dy_loc, weights, a_inv_rows, s_inv)
        core = (lax.axis_index("data") % 2).astype(jnp.int32).reshape(1)
        a_new, s_new = finish(core, res[1], res[2], res[3], res[4], a_old_rows, s_old_rows)
        return res[0], a_new, s_new

    row_spec = P("data", None)
    return jax.shard_map(
        device_step,
        mesh=mesh,
        in_specs=(row_spec, row_spec, P(), row_spec, row_spec, row_spec, P()),
        out_specs=(P(), row_spec, row_spec),
        check_vma=False,
    )
```

```python
import functools
import math
import jax
import jax.numpy as jnp
from jax import lax
from jax.experimental import pallas as pl
from jax.experimental.pallas import tpu as pltpu
from jax.sharding import PartitionSpec as P

F32 = jnp.float32
BF16 = jnp.bfloat16
MESH = pl.DeviceIdType.MESH
PRECISE = lax.Precision.HIGHEST
FACTOR_DECAY = 0.75
GELU_A = math.sqrt(2.0 / math.pi)
GELU_B = GELU_A * 0.044715

D = 1024
BK = 512
HALF = D // 2
EB = 64
PR, PC = 256, 1280


def gelu(z):
    hz = 0.5 * z
    return hz + hz * jnp.tanh(z * (GELU_A + GELU_B * (z * z)))


def gelu_slope(z):
    m = GELU_B * (z * z)
    t = jnp.tanh(z * (GELU_A + m))
    return (0.5 + 0.5 * t) + (0.5 * z) * (1.0 - t * t) * (GELU_A + 3.0 * m)


def rows_dot(a, b):
    return lax.dot_general(a, b, (((0,), (0,)), ((), ())), preferred_element_type=F32)


def add_gram(acc, slot, v):
    c = [slice(256 * j, 256 * (j + 1)) for j in range(4)]
    acc[slot, 0, :, 0:1024] += rows_dot(v[:, c[0]], v)
    acc[slot, 0, :, 1024:1280] += rows_dot(v[:, c[1]], v[:, c[1]])
    acc[slot, 1, :, 0:512] += rows_dot(v[:, c[1]], v[:, 512:])
    acc[slot, 1, :, 512:1024] += rows_dot(v[:, c[2]], v[:, 512:])
    acc[slot, 1, :, 1024:1280] += rows_dot(v[:, c[3]], v[:, c[3]])


class Sems:
    def __init__(self):
        self.n = 0

    def take(self, n=1):
        i = self.n
        self.n += n
        return i


def mega_kernel(nb, x, dy, w, ainv, sinv,
                u, own_a, oth_a, own_s, oth_s, hs, zs, gs, oa, os_, qp, ainv_all, t_all,
                buf, wb, acc_g, acc_p, d_g, d_p, rs, tb, stage, big, ain, ub,
                in_sem, out_sem, w_sem, loc_sem, snd, rcv, gsnd, grcv, asnd, arcv, usnd, urcv):
    dev = lax.axis_index("data")
    k = dev % 2
    c = dev // 2
    cx = c % 2
    cy = c // 2
    partner = 2 * c + (1 - k)
    xn = 2 * (2 * cy + (1 - cx)) + k
    yn = 2 * (2 * (1 - cy) + cx) + k

    def rdma(src, dst, ss, rs, to):
        return pltpu.make_async_remote_copy(src_ref=src, dst_ref=dst, send_sem=ss, recv_sem=rs,
                                            device_id=(to,), device_id_type=MESH)

    def local(src, dst, i):
        return pltpu.make_async_copy(src, dst, loc_sem.at[i])

    class Job:
        def __init__(self, kind, layer, slot):
            o = layer
            self.o, self.dg = o, 3 - o
            self.nx = (o // 2) * 2 + (1 - o % 2)
            self.ny = (1 - o // 2) * 2 + o % 2
            i = layer if kind == "a" else 4 + layer
            self.acc = lambda h: acc_p.at[slot, h]
            self.d, self.q, self.oo = d_p.at[i], qp.at[i], (oa if kind == "a" else os_)
            self.rows, self.ch = PR, 32
            self.s0, self.r0 = 3 * i, 6 * i
            r2 = self.rows // 2
            self.a, self.b = pl.ds(0, r2), pl.ds(r2, r2)

        def d2d(self):
            return rdma(self.acc(1 - k), self.d, snd.at[self.s0], rcv.at[self.r0], partner)

        def start(self):
            self.d2d().start()

        def finish(self):
            self.d2d().wait_recv()

            def add(i, _):
                r = pl.ds(i * self.ch, self.ch)
                self.d[r] = self.d[r] + self.acc(k)[r]
                return 0
            lax.fori_loop(0, self.rows // self.ch, add, 0)
            self.d2d().wait_send()

        def send(self, role, n):
            ss, r = snd.at[self.s0 + 1 + n], self.r0
            d, q, oo, a, b = self.d, self.q, self.oo, self.a, self.b
            if role == "dg":
                return rdma(d.at[b if n else a], q, ss, rcv.at[r + 1], yn if n else xn)
            if role == "nx":
                part = b if n else a
                return rdma(d.at[part], oo.at[0, part], ss, rcv.at[r + 2 + n], xn)
            part = a if n else b
            return rdma(d.at[part], oo.at[1, part], ss, rcv.at[r + 4 + n], yn)

        def hop1(self):
            @pl.when(c == self.dg)
            def _():
                self.send("dg", 0).start()
                self.send("dg", 1).start()

            @pl.when(c == self.nx)
            def _():
                self.send("nx", 0).start()

            @pl.when(c == self.ny)
            def _():
                self.send("ny", 0).start()

        def hop2(self):
            r2 = self.rows // 2

            def go(role, off):
                self.send("dg", 0).wait_recv()
                cp = local(self.q, stage, 0)
                cp.start()
                cp.wait()

                def add(i, _):
                    r = pl.ds(off + i * self.ch, self.ch)
                    self.d[r] = self.d[r] + stage[pl.ds(i * self.ch, self.ch)]
                    return 0
                lax.fori_loop(0, r2 // self.ch, add, 0)
                self.send(role, 1).start()

            @pl.when(c == self.nx)
            def _():
                go("nx", r2)

            @pl.when(c == self.ny)
            def _():
                go("ny", 0)

        def drain(self):
            for role, chip in (("dg", self.dg), ("nx", self.nx), ("ny", self.ny)):
                @pl.when(c == chip)
                def _():
                    self.send(role, 0).wait_send()
                    self.send(role, 1).wait_send()

        def arrive(self):
            @pl.when(c == self.o)
            def _():
                for role in ("nx", "ny"):
                    self.send(role, 0).wait_recv()
                    self.send(role, 1).wait_recv()

    c_x, c_y, c_z = 2 * cy + (1 - cx), 2 * (1 - cy) + cx, 3 - c
    A0, B0 = pl.ds(0, EB), pl.ds(EB, EB)

    class Grad:
        def __init__(self, layer):
            self.l = layer
            self.slot = (3 - layer) % 2
            self.d, self.r = d_g.at[self.slot], rs.at[self.slot]

        def acc(self, h):
            return acc_g.at[self.slot, pl.ds(h * HALF, HALF)]

        def blk(self, chip, part):
            return self.d.at[pl.ds(chip * (2 * EB) + part * EB, EB)]

        def buf(self, n):
            return self.r.at[pl.ds(n * EB, EB)]

        def d2d(self):
            return rdma(self.acc(1 - k), self.d, gsnd.at[self.l, 0], grcv.at[self.l, 0], partner)

        def start(self):
            self.d2d().start()

        def finish(self):
            self.d2d().wait_recv()

            def add(i, _):
                r = pl.ds(i * 64, 64)
                self.d[r] = self.d[r] + self.acc(k)[r]
                return 0
            lax.fori_loop(0, HALF // 64, add, 0)
            self.d2d().wait_send()

        def send(self, n):
            src, dst, to = ((self.blk(c_z, 0), 0, xn), (self.blk(c_z, 1), 1, yn),
                            (self.blk(c_x, 0), 2, xn), (self.blk(c_y, 1), 5, yn),
                            (self.blk(c_y, 0), 4, yn), (self.blk(c_x, 1), 3, xn))[n]
            return rdma(src, self.buf(dst), gsnd.at[self.l, 1 + n], grcv.at[self.l, 1 + n], to)

        def hop1(self):
            for n in range(4):
                self.send(n).start()

        def hop2(self):
            for n, chip, part in ((0, c_y, 0), (1, c_x, 1)):
                self.send(n).wait_recv()
                t = self.blk(chip, part)
                t[...] = t[...] + self.buf(n)[...]
                self.send(4 + n).start()

        def fin(self):
            for n in (2, 3, 4, 5):
                self.send(n).wait_recv()
            for p in (0, 1):
                t = self.blk(c, p)
                t[...] = t[...] + (self.buf(2 + p)[...] + self.buf(4 + p)[...])
            for n in range(6):
                self.send(n).wait_send()

    class Gather:
        def __init__(self, src, dst, i, swap):
            self.src, self.dst, self.swap, self.met = src, dst, swap, False
            self.snd, self.rcv, self.m0 = asnd.at[i], arcv.at[i], 11 + 2 * i

        def own(self, n):
            part, to = ((0, xn), (1, yn), (1, xn), (0, yn))[n]
            r = ((0, 0), (1, 1), (0, 1), (1, 0))[n]
            return rdma(self.src(part), self.dst(c, part), self.snd.at[n], self.rcv.at[2 * r[0] + r[1]], to)

        def rel(self, n):
            chip, part, to = ((c_x, 0, yn), (c_y, 1, xn))[n]
            ref = self.dst(chip, part)
            return rdma(ref, ref, self.snd.at[4 + n], self.rcv.at[4 + part], to)

        def twin(self, n, part):
            dst = self.dst((c, c_x, c_y, c_z)[n], part)
            return rdma(self.src(part) if n == 0 else dst, dst, self.snd.at[6 + 2 * n + part],
                        self.rcv.at[6 + 2 * n + part], partner)

        def mine(self, part):
            return local(self.src(part), self.dst(c, part), self.m0 + part)

        def got(self, n, part):
            ref = self.dst((c, c_x, c_y, c_z)[n], part)
            rdma(ref, ref, self.snd.at[0], self.rcv.at[2 * (n - 1) + part], partner).wait_recv()
            if self.swap:
                self.twin(n, part).start()

        def first(self):
            self.own(0).start()
            self.own(1).start()

        def second(self):
            self.own(2).start()
            self.own(3).start()
            for p in (0, 1):
                self.mine(p).start()
                if self.swap:
                    self.twin(0, p).start()

        def start(self):
            self.first()
            self.second()

        def relay(self):
            self.got(1, 0)
            self.rel(0).start()
            self.got(2, 1)
            self.rel(1).start()

        def rest(self):
            self.got(1, 1)
            self.got(2, 0)
            self.got(3, 0)
            self.got(3, 1)

        def fin(self):
            for n in range(4):
                self.own(n).wait_send()
            for p in (0, 1):
                self.rel(p).wait_send()
                self.mine(p).wait()
                if self.swap:
                    for n in range(4):
                        self.twin(n, p).wait_send()
                        if n or not self.met:
                            self.twin(n, p).wait_recv()

        def meet(self):
            self.met = True
            for p in (0, 1):
                self.twin(0, p).wait_recv()

    slots_p = {"a0": 0, "s3": 1, "a1": 2, "a2": 0, "a3": 1, "s2": 2, "s1": 0, "s0": 1}
    job = {n: Job(n[0], int(n[1]), s) for n, s in slots_p.items()}
    for l in range(4):
        job[f"g{l}"] = Grad(l)

    def t_part(l):
        return lambda part: tb.at[(3 - l) % 2, pl.ds(part * EB, EB)]

    def t_rows(l):
        return lambda chip, part: t_all.at[l, pl.ds(k * HALF + chip * (2 * EB) + part * EB, EB)]

    for l in range(4):
        job[f"t{l}"] = Gather(t_part(l), t_rows(l), l, True)
    job["i"] = Gather(lambda part: ainv.at[pl.ds(part * (HALF // 2), HALF // 2)],
                      lambda chip, part: ainv_all.at[chip, pl.ds(part * (HALF // 2), HALF // 2)],
                      4, False)

    def ev(what, *names):
        return [getattr(job[n], what) for n in names]

    def load(srcs, i, slot):
        return [pltpu.make_async_copy(s.at[pl.ds(i * BK, BK)], buf.at[j, slot], in_sem.at[j, slot])
                for j, s in enumerate(srcs)]

    def phase(srcs, dsts, body, hooks, zero, nxt, w_next=None):
        def step(i, _):
            slot = i % 2

            @pl.when(i + 1 < nb)
            def _():
                for cp in load(srcs, i + 1, 1 - slot):
                    cp.start()
            if nxt is not None:
                @pl.when(i + 1 == nb)
                def _():
                    for cp in load(nxt, 0, 1 - slot):
                        cp.start()
            for cp in load(srcs, i, slot):
                cp.wait()

            def store(i):
                return [pltpu.make_async_copy(buf.at[3 - j, slot], t.at[pl.ds(i * BK, BK)], out_sem.at[j, slot])
                        for j, t in enumerate(dsts)]
            if dsts:
                @pl.when(i >= 2)
                def _():
                    for cp in store(i - 2):
                        cp.wait()

            @pl.when(i == 0)
            def _():
                for z in zero:
                    z[...] = jnp.zeros(z.shape, F32)
            for at in sorted(hooks):
                @pl.when(i == at)
                def _():
                    for f in hooks[at]:
                        f()
            body([buf.at[j, slot] for j in range(len(srcs))], [buf.at[3 - j, slot] for j in range(len(dsts))])
            for cp in store(i):
                cp.start()
            return 0
        lax.fori_loop(0, nb, step, 0)
        for back in (2, 1):
            for j, t in enumerate(dsts):
                i = nb - back
                pltpu.make_async_copy(buf.at[3 - j, i % 2], t.at[pl.ds(i * BK, BK)], out_sem.at[j, i % 2]).wait()

    def w_copy(l, slot):
        return pltpu.make_async_copy(w.at[l], wb.at[slot], w_sem.at[slot])

    def fwd_body(wslot, pslot, extra=None):
        def body(ins, outs):
            v = ins[0][...]
            for r in (slice(0, BK // 2), slice(BK // 2, BK)):
                z = jnp.dot(ins[0][r], wb[wslot], preferred_element_type=F32).astype(BF16)
                outs[0][r] = z
                outs[1][r] = gelu(z.astype(F32)).astype(BF16)
            add_gram(acc_p, pslot, v)
            if extra is not None:
                add_gram(acc_p, extra, ins[1][...])
        return body

    def bwd_body(wslot, gslot, pslot, stream=0):
        def body(ins, outs):
            g = ins[0][...]
            for r in (slice(0, BK // 2), slice(BK // 2, BK)):
                d = lax.dot_general(ins[0][r], wb[wslot], (((1,), (1,)), ((), ())),
                                    preferred_element_type=F32).astype(BF16)
                outs[0][r] = (d.astype(F32) * gelu_slope(ins[2][r].astype(F32))).astype(BF16)
            acc_g[gslot] += rows_dot(ins[1][...], g)
            add_gram(acc_p, pslot, ins[stream][...])
        return body

    def cross_body(gslot, pslot):
        def body(ins, outs):
            g = ins[0][...]
            acc_g[gslot] += rows_dot(ins[1][...], g)
            add_gram(acc_p, pslot, g)
        return body

    def precise_dot(lhs, out):
        out[...] = jnp.zeros(out.shape, F32)

        def part(i, _):
            r = pl.ds(pl.multiple_of(i * 256, 256), 256)
            out[...] += jnp.dot(lhs[:, r], big[r], precision=PRECISE, preferred_element_type=F32)
            return 0
        lax.fori_loop(0, D // 256, part, 0)

    def t_stage(l):
        def go():
            cp = local(sinv.at[l], big, 4)
            cp.start()
            job[f"g{l}"].fin()
            cp.wait()
            t = tb.at[(3 - l) % 2]
            precise_dot(job[f"g{l}"].d.at[pl.ds(c * (2 * EB), 2 * EB)], t)
            t[...] = t[...] * (1.0 / (nb * BK * 8))
            job[f"t{l}"].start()
        return go

    def u_out(l):
        half = u.at[l, pl.ds(k * HALF, HALF)]
        return rdma(ub, half, usnd.at[l], urcv.at[l], partner), local(ub, half, 5)

    def u_stage(l, prev=None):
        job[f"t{l}"].fin()
        cps = [local(t_all.at[l], big, 4), local(ainv_all.at[l], ain, 6)]
        for cp in cps:
            cp.start()
        if prev is not None:
            u_done(prev)
        for cp in cps:
            cp.wait()

        precise_dot(ain, ub)
        for cp in u_out(l):
            cp.start()

    def u_done(l):
        there, here = u_out(l)
        there.wait()
        here.wait()

    ap = [acc_p.at[i] for i in range(3)]
    ag = [acc_g.at[i] for i in range(2)]
    h = [x, hs.at[0], hs.at[1], hs.at[2]]
    g = [gs.at[0], gs.at[1], gs.at[2], dy]
    s_f1, s_f2, s_f3 = [h[0], dy], [h[1]], [h[2]]
    s_b4, s_b3, s_b2 = [g[3], h[3], zs.at[2]], [g[2], h[2], zs.at[1]], [g[1], h[1], zs.at[0]]
    s_l1 = [g[0], h[0]]

    def run(evs):
        for f in evs:
            f()

    w_copy(0, 0).start()
    for cp in load(s_f1, 0, 0):
        cp.start()
    run(ev("first", "i"))
    w_copy(0, 0).wait()
    w_copy(1, 1).start()
    phase(s_f1, [zs.at[0], hs.at[0]], fwd_body(0, 0, 1), {}, [ap[0], ap[1]], s_f2)
    w_copy(1, 1).wait()
    w_copy(2, 0).start()
    phase(s_f2, [zs.at[1], hs.at[1]], fwd_body(1, 2),
          {0: ev("start", "a0", "s3"), 1: ev("finish", "a0", "s3") + ev("hop1", "a0", "s3"),
           7: ev("hop2", "a0", "s3")}, [ap[2]], s_f3)
    w_copy(2, 0).wait()
    w_copy(3, 1).start()
    phase(s_f3, [zs.at[2], hs.at[2]], fwd_body(0, 0),
          {0: ev("start", "a1"), 1: ev("finish", "a1") + ev("hop1", "a1"), 2: ev("second", "i")}, [ap[0]], None)
    for cp in load(s_b4, 0, 0):
        cp.start()
    w_copy(3, 1).wait()
    w_copy(2, 0).start()
    phase(s_b4, [gs.at[2]], bwd_body(1, 0, 1, 1),
          {0: ev("start", "a2"), 1: ev("finish", "a2") + ev("hop1", "a2"), 3: ev("hop2", "a1"),
           4: ev("relay", "i"), 7: ev("hop2", "a2")},
          [ag[0], ap[1]], s_b3)
    w_copy(2, 0).wait()
    w_copy(1, 1).start()
    phase(s_b3, [gs.at[1]], bwd_body(0, 1, 2),
          {0: ev("start", "g3", "a3"), 1: ev("finish", "g3") + ev("hop1", "g3") + ev("finish", "a3"),
           2: ev("hop1", "a3"), 5: ev("hop2", "g3")}, [ag[1], ap[2]], s_b2)
    w_copy(1, 1).wait()
    phase(s_b2, [gs.at[0]], bwd_body(1, 0, 0),
          {0: ev("start", "g2", "s2"), 1: [t_stage(3)] + ev("finish", "g2") + ev("hop1", "g2"),
           2: ev("finish", "s2") + ev("hop2", "a3"), 3: ev("relay", "t3"), 4: ev("hop1", "s2"),
           5: ev("hop2", "g2"), 7: ev("rest", "t3")}, [ag[0], ap[0]], s_l1)
    run(ev("rest", "i") + ev("fin", "i"))
    u_stage(3)
    phase(s_l1, [], cross_body(1, 1),
          {0: ev("start", "g1", "s1") + [t_stage(2)], 1: ev("finish", "g1") + ev("hop1", "g1") + ev("finish", "s1"),
           4: ev("relay", "t2"), 6: ev("hop2", "s2")},
          [ag[1], ap[1]], None)
    run(ev("meet", "t2") + ev("start", "g0", "s0") + ev("hop2", "g1") + ev("finish", "g0", "s0") + ev("hop1", "g0")
        + ev("rest", "t2"))
    u_stage(2, 3)
    t_stage(1)()
    run(ev("hop2", "g0") + ev("relay", "t1") + ev("hop1", "s1", "s0") + ev("rest", "t1"))
    t_stage(0)()
    u_stage(1, 2)
    run(ev("relay", "t0") + ev("hop2", "s1", "s0") + ev("rest", "t0"))
    u_stage(0, 1)

    for n in ("a0", "a1", "a2", "a3", "s3", "s2", "s1", "s0"):
        job[n].drain()
        job[n].arrive()
    for j, src in enumerate((oa, os_)):
        local(src, acc_p.at[j], 7 + j).start()
    fin = []
    for j, (src, mine, other) in enumerate(((oa, own_a, oth_a), (os_, own_s, oth_s))):
        local(src, acc_p.at[j], 7 + j).wait()

        def add(i, _):
            r = pl.ds(i * 32, 32)
            d_p[4 * j + c, r] = d_p[4 * j + c, r] + (acc_p[j, 0, r] + acc_p[j, 1, r])
            return 0
        lax.fori_loop(0, PR // 32, add, 0)
        own = d_p.at[4 * j + c]
        fin.append((rdma(own, other, usnd.at[4 + j], urcv.at[4 + j], partner), local(own, mine, 9 + j)))
        for cp in fin[-1]:
            cp.start()
    for r, cp in fin:
        r.wait()
        cp.wait()
    u_done(0)


def mega(x, dy, w, ainv, sinv):
    n = x.shape[0]
    nb = n // BK
    hbm = pl.BlockSpec(memory_space=pltpu.HBM)

    def sh(s, t=F32):
        return jax.ShapeDtypeStruct(s, t)
    half = (PR, PC)
    outs = [sh((4, D, D)), sh(half), sh(half), sh(half), sh(half),
            sh((3, n, D), BF16), sh((3, n, D), BF16), sh((3, n, D), BF16),
            sh((2,) + half), sh((2,) + half), sh((8, PR // 2, PC)), sh((4, HALF, D)), sh((4, D, D))]
    dma = pltpu.SemaphoreType.DMA
    return pl.pallas_call(
        functools.partial(mega_kernel, nb),
        out_shape=outs,
        in_specs=[hbm] * 5,
        out_specs=[hbm] * len(outs),
        scratch_shapes=[
            pltpu.VMEM((4, 2, BK, D), BF16), pltpu.VMEM((2, D, D), BF16),
            pltpu.VMEM((2, D, D), F32), pltpu.VMEM((3, 2) + half, F32),
            pltpu.VMEM((2, HALF, D), F32), pltpu.VMEM((8,) + half, F32), pltpu.VMEM((2, 6 * EB, D), F32), pltpu.VMEM((2, 2 * EB, D), F32),
            pltpu.VMEM((PR // 2, PC), F32), pltpu.VMEM((D, D), F32), pltpu.VMEM((HALF, D), F32),
            pltpu.VMEM((HALF, D), F32),
            dma((3, 2)), dma((2, 2)), dma((2,)), dma((21,)), dma((24,)), dma((48,)), dma((4, 7)), dma((4, 7)),
            dma((5, 14)), dma((5, 14)), dma((6,)), dma((6,)),
        ],
        compiler_params=pltpu.CompilerParams(has_side_effects=True, vmem_limit_bytes=67_043_328),
        name="kfac",
    )(x, dy, w, ainv, sinv)


def finish_kernel(ka, oa, ob, os_, ot, a_old, s_old, a_new, s_new, p, old, new, sem, out_sem):
    scale = (1.0 - FACTOR_DECAY) / (8 * 4096)
    ins = [pltpu.make_async_copy(s, t, sem.at[n]) for n, (s, t) in enumerate(
        ((oa, p.at[0]), (ob, p.at[1]), (a_old, old.at[0]), (os_, p.at[2]), (ot, p.at[3]), (s_old, old.at[1])))]
    outs = [pltpu.make_async_copy(new.at[n], t, out_sem.at[n]) for n, t in enumerate((a_new, s_new))]
    for cp in ins:
        cp.start()

    def blend(n, r, cs, v):
        new[n, r, cs] = FACTOR_DECAY * old[n, r, cs] + scale * v
    c = [slice(256 * j, 256 * (j + 1)) for j in range(5)]
    for n in range(2):
        for cp in ins[3 * n:3 * n + 3]:
            cp.wait()
        own, oth = p.at[2 * n], p.at[2 * n + 1]

        @pl.when(ka[0] == 0)
        def _():
            blend(n, c[0], slice(0, 1024), own[:, 0:1024])
            blend(n, c[1], c[0], own[:, c[1]].T)
            blend(n, c[1], c[1], own[:, c[4]])
            blend(n, c[1], slice(512, 1024), oth[:, 0:512])

        @pl.when(ka[0] == 1)
        def _():
            blend(n, c[0], c[0], oth[:, c[2]].T)
            blend(n, c[0], c[1], own[:, c[0]].T)
            blend(n, c[0], slice(512, 1024), own[:, 512:1024])
            blend(n, c[1], c[0], oth[:, c[3]].T)
            blend(n, c[1], c[1], own[:, c[1]].T)
            blend(n, c[1], c[2], own[:, c[3]].T)
            blend(n, c[1], c[3], own[:, c[4]])
        outs[n].start()
    for cp in outs:
        cp.wait()


def finish(core, oa, ob, os_, ot, a_old, s_old):
    sd = jax.ShapeDtypeStruct((HALF, D), F32)
    hbm = pl.BlockSpec(memory_space=pltpu.HBM)
    dma = pltpu.SemaphoreType.DMA
    return pl.pallas_call(
        finish_kernel,
        out_shape=[sd, sd],
        in_specs=[pl.BlockSpec(memory_space=pltpu.SMEM)] + [hbm] * 6,
        out_specs=[hbm] * 2,
        scratch_shapes=[pltpu.VMEM((4, PR, PC), F32), pltpu.VMEM((2, HALF, D), F32), pltpu.VMEM((2, HALF, D), F32),
                        dma((6,)), dma((2,))],
        compiler_params=pltpu.CompilerParams(vmem_limit_bytes=67_043_328),
        name="blend",
    )(core, oa, ob, os_, ot, a_old, s_old)


def solution(mesh):
    def device_step(x_loc, dy_loc, weights, a_old_rows, s_old_rows, a_inv_rows, s_inv):
        res = mega(x_loc, dy_loc, weights, a_inv_rows, s_inv)
        core = (lax.axis_index("data") % 2).astype(jnp.int32).reshape(1)
        a_new, s_new = finish(core, res[1], res[2], res[3], res[4], a_old_rows, s_old_rows)
        return res[0], a_new, s_new

    row_spec = P("data", None)
    return jax.shard_map(
        device_step,
        mesh=mesh,
        in_specs=(row_spec, row_spec, P(), row_spec, row_spec, row_spec, P()),
        out_specs=(P(), row_spec, row_spec),
        check_vma=False,
    )
```

```python
import functools
import math
import jax
import jax.numpy as jnp
from jax import lax
from jax.experimental import pallas as pl
from jax.experimental.pallas import tpu as pltpu
from jax.sharding import PartitionSpec as P

F32 = jnp.float32
BF16 = jnp.bfloat16
MESH = pl.DeviceIdType.MESH
PRECISE = lax.Precision.HIGHEST
FACTOR_DECAY = 0.75
GELU_A = math.sqrt(2.0 / math.pi)
GELU_B = GELU_A * 0.044715

D = 1024
BK = 512
QUARTER = D // 4
HALF = D // 2
EIGHTH = D // 8
EB = EIGHTH // 2
BLOCKS = [slice(j, j + 256) for j in range(0, 1280, 256)]
PR, PC = 256, 1280


def gelu(z):
    hz = 0.5 * z
    return hz + hz * jnp.tanh(z * (GELU_A + GELU_B * (z * z)))


def gelu_slope(z):
    m = GELU_B * (z * z)
    t = jnp.tanh(z * (GELU_A + m))
    return (0.5 + 0.5 * t) + (0.5 * z) * (1.0 - t * t) * (GELU_A + 3.0 * m)


def rows_dot(a, b):
    return lax.dot_general(a, b, (((0,), (0,)), ((), ())), preferred_element_type=F32)


def add_gram(acc, slot, v):
    c = BLOCKS
    acc[slot, 0, :, :D] += rows_dot(v[:, c[0]], v)
    acc[slot, 0, :, D:] += rows_dot(v[:, c[1]], v[:, c[1]])
    acc[slot, 1, :, :HALF] += rows_dot(v[:, c[1]], v[:, HALF:])
    acc[slot, 1, :, HALF:D] += rows_dot(v[:, c[2]], v[:, HALF:])
    acc[slot, 1, :, D:] += rows_dot(v[:, c[3]], v[:, c[3]])


class Sems:
    def __init__(self):
        self.n = 0

    def take(self, n=1):
        i = self.n
        self.n += n
        return i


def mega_kernel(nb, x, dy, w, ainv, sinv,
                u, own_a, oth_a, own_s, oth_s, hs, zs, gs, oa, os_, qp, ainv_all, t_all,
                buf, wb, acc_g, acc_p, d_g, d_p, rs, tb, stage, big, ain, ub,
                in_sem, out_sem, w_sem, loc_sem, snd, rcv, gsnd, grcv, asnd, arcv, usnd, urcv):
    dev = lax.axis_index("data")
    k = dev % 2
    c = dev // 2
    cx = c % 2
    cy = c // 2
    partner = 2 * c + (1 - k)
    xn = 2 * (2 * cy + (1 - cx)) + k
    yn = 2 * (2 * (1 - cy) + cx) + k

    def rdma(src, dst, ss, rs, to):
        return pltpu.make_async_remote_copy(src_ref=src, dst_ref=dst, send_sem=ss, recv_sem=rs,
                                            device_id=(to,), device_id_type=MESH)

    def local(src, dst, i):
        return pltpu.make_async_copy(src, dst, loc_sem.at[i])

    class Job:
        def __init__(self, kind, layer, slot):
            o = layer
            self.o, self.dg = o, 3 - o
            self.nx = (o // 2) * 2 + (1 - o % 2)
            self.ny = (1 - o // 2) * 2 + o % 2
            i = layer if kind == "a" else 4 + layer
            self.acc = lambda h: acc_p.at[slot, h]
            self.d, self.q, self.oo = d_p.at[i], qp.at[i], (oa if kind == "a" else os_)
            self.rows, self.ch = PR, 32
            self.s0, self.r0 = 3 * i, 6 * i
            r2 = self.rows // 2
            self.a, self.b = pl.ds(0, r2), pl.ds(r2, r2)

        def d2d(self):
            return rdma(self.acc(1 - k), self.d, snd.at[self.s0], rcv.at[self.r0], partner)

        def start(self):
            self.d2d().start()

        def finish(self):
            self.d2d().wait_recv()

            def add(i, _):
                r = pl.ds(i * self.ch, self.ch)
                self.d[r] = self.d[r] + self.acc(k)[r]
                return 0
            lax.fori_loop(0, self.rows // self.ch, add, 0)
            self.d2d().wait_send()

        def send(self, role, n):
            ss, r = snd.at[self.s0 + 1 + n], self.r0
            d, q, oo, a, b = self.d, self.q, self.oo, self.a, self.b
            if role == "dg":
                return rdma(d.at[b if n else a], q, ss, rcv.at[r + 1], yn if n else xn)
            if role == "nx":
                part = b if n else a
                return rdma(d.at[part], oo.at[0, part], ss, rcv.at[r + 2 + n], xn)
            part = a if n else b
            return rdma(d.at[part], oo.at[1, part], ss, rcv.at[r + 4 + n], yn)

        def hop1(self):
            @pl.when(c == self.dg)
            def _():
                self.send("dg", 0).start()
                self.send("dg", 1).start()

            @pl.when(c == self.nx)
            def _():
                self.send("nx", 0).start()

            @pl.when(c == self.ny)
            def _():
                self.send("ny", 0).start()

        def hop2(self):
            r2 = self.rows // 2

            def go(role, off):
                self.send("dg", 0).wait_recv()
                cp = local(self.q, stage, 0)
                cp.start()
                cp.wait()

                def add(i, _):
                    r = pl.ds(off + i * self.ch, self.ch)
                    self.d[r] = self.d[r] + stage[pl.ds(i * self.ch, self.ch)]
                    return 0
                lax.fori_loop(0, r2 // self.ch, add, 0)
                self.send(role, 1).start()

            @pl.when(c == self.nx)
            def _():
                go("nx", r2)

            @pl.when(c == self.ny)
            def _():
                go("ny", 0)

        def drain(self):
            for role, chip in (("dg", self.dg), ("nx", self.nx), ("ny", self.ny)):
                @pl.when(c == chip)
                def _():
                    self.send(role, 0).wait_send()
                    self.send(role, 1).wait_send()

        def arrive(self):
            @pl.when(c == self.o)
            def _():
                for role in ("nx", "ny"):
                    self.send(role, 0).wait_recv()
                    self.send(role, 1).wait_recv()

    c_x, c_y, c_z = 2 * cy + (1 - cx), 2 * (1 - cy) + cx, 3 - c
    A0, B0 = pl.ds(0, EB), pl.ds(EB, EB)

    class Grad:
        def __init__(self, layer):
            self.l = layer
            self.slot = (3 - layer) % 2
            self.d, self.r = d_g.at[self.slot], rs.at[self.slot]

        def acc(self, h):
            return acc_g.at[self.slot, pl.ds(h * HALF, HALF)]

        def blk(self, chip, part):
            return self.d.at[pl.ds(chip * (EIGHTH) + part * EB, EB)]

        def buf(self, n):
            return self.r.at[pl.ds(n * EB, EB)]

        def d2d(self):
            return rdma(self.acc(1 - k), self.d, gsnd.at[self.l, 0], grcv.at[self.l, 0], partner)

        def start(self):
            self.d2d().start()

        def finish(self):
            self.d2d().wait_recv()

            def add(i, _):
                r = pl.ds(i * 64, 64)
                self.d[r] = self.d[r] + self.acc(k)[r]
                return 0
            lax.fori_loop(0, HALF // 64, add, 0)
            self.d2d().wait_send()

        def send(self, n):
            src, dst, to = ((self.blk(c_z, 0), 0, xn), (self.blk(c_z, 1), 1, yn),
                            (self.blk(c_x, 0), 2, xn), (self.blk(c_y, 1), 5, yn),
                            (self.blk(c_y, 0), 4, yn), (self.blk(c_x, 1), 3, xn))[n]
            return rdma(src, self.buf(dst), gsnd.at[self.l, 1 + n], grcv.at[self.l, 1 + n], to)

        def hop1(self):
            for n in range(4):
                self.send(n).start()

        def hop2(self):
            for n, chip, part in ((0, c_y, 0), (1, c_x, 1)):
                self.send(n).wait_recv()
                t = self.blk(chip, part)
                t[...] = t[...] + self.buf(n)[...]
                self.send(4 + n).start()

        def fin(self):
            for n in (2, 3, 4, 5):
                self.send(n).wait_recv()
            for p in (0, 1):
                t = self.blk(c, p)
                t[...] = t[...] + (self.buf(2 + p)[...] + self.buf(4 + p)[...])
            for n in range(6):
                self.send(n).wait_send()

    class Gather:
        def __init__(self, src, dst, i, swap):
            self.src, self.dst, self.swap, self.met = src, dst, swap, False
            self.snd, self.rcv, self.m0 = asnd.at[i], arcv.at[i], 11 + 2 * i

        def own(self, n):
            part, to = ((0, xn), (1, yn), (1, xn), (0, yn))[n]
            r = ((0, 0), (1, 1), (0, 1), (1, 0))[n]
            return rdma(self.src(part), self.dst(c, part), self.snd.at[n], self.rcv.at[2 * r[0] + r[1]], to)

        def rel(self, n):
            chip, part, to = ((c_x, 0, yn), (c_y, 1, xn))[n]
            ref = self.dst(chip, part)
            return rdma(ref, ref, self.snd.at[4 + n], self.rcv.at[4 + part], to)

        def twin(self, n, part):
            dst = self.dst((c, c_x, c_y, c_z)[n], part)
            return rdma(self.src(part) if n == 0 else dst, dst, self.snd.at[6 + 2 * n + part],
                        self.rcv.at[6 + 2 * n + part], partner)

        def mine(self, part):
            return local(self.src(part), self.dst(c, part), self.m0 + part)

        def got(self, n, part):
            ref = self.dst((c, c_x, c_y, c_z)[n], part)
            rdma(ref, ref, self.snd.at[0], self.rcv.at[2 * (n - 1) + part], partner).wait_recv()
            if self.swap:
                self.twin(n, part).start()

        def first(self):
            self.own(0).start()
            self.own(1).start()

        def second(self):
            self.own(2).start()
            self.own(3).start()
            for p in (0, 1):
                self.mine(p).start()
                if self.swap:
                    self.twin(0, p).start()

        def start(self):
            self.first()
            self.second()

        def relay(self):
            self.got(1, 0)
            self.rel(0).start()
            self.got(2, 1)
            self.rel(1).start()

        def rest(self):
            self.got(1, 1)
            self.got(2, 0)
            self.got(3, 0)
            self.got(3, 1)

        def fin(self):
            for n in range(4):
                self.own(n).wait_send()
            for p in (0, 1):
                self.rel(p).wait_send()
                self.mine(p).wait()
                if self.swap:
                    for n in range(4):
                        self.twin(n, p).wait_send()
                        if n or not self.met:
                            self.twin(n, p).wait_recv()

        def meet(self):
            self.met = True
            for p in (0, 1):
                self.twin(0, p).wait_recv()

    slots_p = dict(a0=0, s3=1, a1=2, a2=0, a3=1, s2=2, s1=0, s0=1)
    job = {n: Job(n[0], int(n[1]), s) for n, s in slots_p.items()}
    for l in range(4):
        job[f"g{l}"] = Grad(l)

    def t_part(l):
        return lambda part: tb.at[(3 - l) % 2, pl.ds(part * EB, EB)]

    def t_rows(l):
        return lambda chip, part: t_all.at[l, pl.ds(k * HALF + chip * (EIGHTH) + part * EB, EB)]

    for l in range(4):
        job[f"t{l}"] = Gather(t_part(l), t_rows(l), l, True)
    job["i"] = Gather(lambda part: ainv.at[pl.ds(part * QUARTER, QUARTER)],
                      lambda chip, part: ainv_all.at[chip, pl.ds(part * QUARTER, QUARTER)],
                      4, False)

    def ev(what, *names):
        return [getattr(job[n], what) for n in names]

    def run(evs):
        for f in evs:
            f()

    def load(srcs, i, slot):
        return [pltpu.make_async_copy(s.at[pl.ds(i * BK, BK)], buf.at[j, slot], in_sem.at[j, slot])
                for j, s in enumerate(srcs)]

    def phase(srcs, dsts, body, hooks, zero, nxt, w_next=None):
        def step(i, _):
            slot = i % 2

            @pl.when(i + 1 < nb)
            def _():
                for cp in load(srcs, i + 1, 1 - slot):
                    cp.start()
            if nxt is not None:
                @pl.when(i + 1 == nb)
                def _():
                    for cp in load(nxt, 0, 1 - slot):
                        cp.start()
            for cp in load(srcs, i, slot):
                cp.wait()

            def store(i):
                return [pltpu.make_async_copy(buf.at[3 - j, slot], t.at[pl.ds(i * BK, BK)], out_sem.at[j, slot])
                        for j, t in enumerate(dsts)]
            if dsts:
                @pl.when(i >= 2)
                def _():
                    for cp in store(i - 2):
                        cp.wait()

            @pl.when(i == 0)
            def _():
                for z in zero:
                    z[...] = jnp.zeros(z.shape, F32)
            for at, evs in enumerate(hooks):
                if evs:
                    @pl.when(i == at)
                    def _():
                        run(evs)
            body([buf.at[j, slot] for j in range(len(srcs))], [buf.at[3 - j, slot] for j in range(len(dsts))])
            for cp in store(i):
                cp.start()
            return 0
        lax.fori_loop(0, nb, step, 0)
        for back in (2, 1):
            for j, t in enumerate(dsts):
                i = nb - back
                pltpu.make_async_copy(buf.at[3 - j, i % 2], t.at[pl.ds(i * BK, BK)], out_sem.at[j, i % 2]).wait()

    def w_copy(l, slot):
        return pltpu.make_async_copy(w.at[l], wb.at[slot], w_sem.at[slot])

    halves = (slice(0, BK // 2), slice(BK // 2, BK))

    def fwd_body(wslot, *slots):
        def body(ins, outs):
            for r in halves:
                z = jnp.dot(ins[0][r], wb[wslot], preferred_element_type=F32).astype(BF16)
                outs[0][r] = z
                outs[1][r] = gelu(z.astype(F32)).astype(BF16)
            for j, p in enumerate(slots):
                add_gram(acc_p, p, ins[j][...])
        return body

    def bwd_body(wslot, gslot, new, old=None):
        def body(ins, outs):
            for r in halves:
                d = lax.dot_general(ins[0][r], wb[wslot], (((1,), (1,)), ((), ())),
                                    preferred_element_type=F32).astype(BF16)
                outs[0][r] = (d.astype(F32) * gelu_slope(ins[2][r].astype(F32))).astype(BF16)
            acc_g[gslot] += rows_dot(ins[1][...], ins[0][...])
            add_gram(acc_p, new, outs[0][...])
            if old is not None:
                add_gram(acc_p, old, ins[1][...])
        return body

    def cross_body(gslot):
        def body(ins, outs):
            acc_g[gslot] += rows_dot(ins[1][...], ins[0][...])
        return body

    def precise_dot(lhs, out):
        out[...] = jnp.zeros(out.shape, F32)

        def part(i, _):
            r = pl.ds(pl.multiple_of(i * 256, 256), 256)
            out[...] += jnp.dot(lhs[:, r], big[r], precision=PRECISE, preferred_element_type=F32)
            return 0
        lax.fori_loop(0, D // 256, part, 0)

    def t_stage(l):
        def go():
            cp = local(sinv.at[l], big, 4)
            cp.start()
            job[f"g{l}"].fin()
            cp.wait()
            t = tb.at[(3 - l) % 2]
            precise_dot(job[f"g{l}"].d.at[pl.ds(c * (EIGHTH), EIGHTH)], t)
            t[...] = t[...] * (1.0 / (nb * BK * 8))
            job[f"t{l}"].start()
        return go

    def u_out(l):
        half = u.at[l, pl.ds(k * HALF, HALF)]
        return rdma(ub, half, usnd.at[l], urcv.at[l], partner), local(ub, half, 5)

    def u_stage(l, prev=None):
        job[f"t{l}"].fin()
        cps = [local(t_all.at[l], big, 4), local(ainv_all.at[l], ain, 6)]
        for cp in cps:
            cp.start()
        if prev is not None:
            u_done(prev)
        for cp in cps:
            cp.wait()

        precise_dot(ain, ub)
        for cp in u_out(l):
            cp.start()

    def u_done(l):
        there, here = u_out(l)
        there.wait()
        here.wait()

    ap = [acc_p.at[i] for i in range(3)]
    ag = [acc_g.at[i] for i in range(2)]
    h = [x, hs.at[0], hs.at[1], hs.at[2]]
    g = [gs.at[0], gs.at[1], gs.at[2], dy]
    s_f1, s_f2, s_f3 = [h[0], dy], [h[1]], [h[2]]
    s_b4, s_b3, s_b2 = ([g[l + 1], h[l + 1], zs.at[l]] for l in (2, 1, 0))
    s_l1 = [g[0], h[0]]

    w_copy(0, 0).start()
    for cp in load(s_f1, 0, 0):
        cp.start()
    run(ev("first", "i"))
    w_copy(0, 0).wait()
    w_copy(1, 1).start()
    no = []
    phase(s_f1, [zs.at[0], hs.at[0]], fwd_body(0, 0, 1), no, [ap[0], ap[1]], s_f2)
    w_copy(1, 1).wait()
    w_copy(2, 0).start()
    phase(s_f2, [zs.at[1], hs.at[1]], fwd_body(1, 2),
          [ev("start", "a0", "s3"), ev("finish", "a0", "s3") + ev("hop1", "a0", "s3"),
           no, no, no, no, no, ev("hop2", "a0", "s3")], [ap[2]], s_f3)
    w_copy(2, 0).wait()
    w_copy(3, 1).start()
    phase(s_f3, [zs.at[2], hs.at[2]], fwd_body(0, 0),
          [ev("start", "a1"), ev("finish", "a1") + ev("hop1", "a1"), ev("second", "i")], [ap[0]], None)
    for cp in load(s_b4, 0, 0):
        cp.start()
    w_copy(3, 1).wait()
    w_copy(2, 0).start()
    phase(s_b4, [gs.at[2]], bwd_body(1, 0, 2, 1),
          [ev("start", "a2"), ev("finish", "a2") + ev("hop1", "a2"), ev("hop2", "a1"),
           ev("relay", "i"), no, ev("hop2", "a2")], [ag[0], ap[1], ap[2]], s_b3)
    w_copy(2, 0).wait()
    w_copy(1, 1).start()
    phase(s_b3, [gs.at[1]], bwd_body(0, 1, 0),
          [ev("start", "g3", "a3"), ev("finish", "g3") + ev("hop1", "g3") + ev("start", "s2") + ev("finish", "a3"),
           ev("finish", "s2"), no, ev("hop2", "g3"), ev("hop1", "a3", "s2")], [ag[1], ap[0]], s_b2)
    w_copy(1, 1).wait()
    phase(s_b2, [gs.at[0]], bwd_body(1, 0, 1),
          [ev("start", "g2", "s1"), [t_stage(3)] + ev("finish", "g2") + ev("hop1", "g2") + ev("finish", "s1"),
           no, ev("relay", "t3"), ev("hop2", "g2"), ev("hop2", "a3", "s2"), no,
           ev("rest", "t3")], [ag[0], ap[1]], s_l1)
    phase(s_l1, [], cross_body(1),
          [ev("meet", "t3") + ev("start", "g1", "s0") + [t_stage(2)],
           ev("finish", "g1") + ev("hop1", "g1") + ev("finish", "s0"), no, no, no, no, no, ev("relay", "t2")],
          [ag[1]], None)
    run(ev("meet", "t2") + ev("start", "g0") + ev("hop2", "g1") + ev("finish", "g0") + ev("hop1", "g0")
        + ev("hop1", "s1") + ev("rest", "i") + ev("fin", "i"))
    u_stage(3)
    t_stage(1)()
    run(ev("hop2", "g0") + ev("relay", "t1") + ev("rest", "t2") + ev("hop1", "s0"))
    u_stage(2, 3)
    t_stage(0)()
    run(ev("hop2", "s1") + ev("rest", "t1"))
    u_stage(1, 2)
    run(ev("relay", "t0") + ev("hop2", "s0") + ev("rest", "t0"))
    u_stage(0, 1)

    for n in slots_p:
        job[n].drain()
        job[n].arrive()
    for j, src in enumerate((oa, os_)):
        local(src, acc_p.at[j], 7 + j).start()
    fin = []
    for j, (src, mine, other) in enumerate(((oa, own_a, oth_a), (os_, own_s, oth_s))):
        local(src, acc_p.at[j], 7 + j).wait()

        def add(i, _):
            r = pl.ds(i * 32, 32)
            d_p[4 * j + c, r] = d_p[4 * j + c, r] + (acc_p[j, 0, r] + acc_p[j, 1, r])
            return 0
        lax.fori_loop(0, PR // 32, add, 0)
        own = d_p.at[4 * j + c]
        fin.append((rdma(own, other, usnd.at[4 + j], urcv.at[4 + j], partner), local(own, mine, 9 + j)))
        for cp in fin[-1]:
            cp.start()
    for r, cp in fin:
        r.wait()
        cp.wait()
    u_done(0)


def mega(x, dy, w, ainv, sinv):
    n = x.shape[0]
    nb = n // BK
    hbm = pl.BlockSpec(memory_space=pltpu.HBM)

    def sh(s, t=F32):
        return jax.ShapeDtypeStruct(s, t)
    half = (PR, PC)
    one, pair, rows = sh(half), sh((2,) + half), sh((3, n, D), BF16)
    outs = [sh((4, D, D)), one, one, one, one,
            rows, rows, rows,
            pair, pair, sh((8, PR // 2, PC)), sh((4, HALF, D)), sh((4, D, D))]
    dma = pltpu.SemaphoreType.DMA
    two, six, seven, many = dma((2,)), dma((6,)), dma((4, 7)), dma((5, 14))
    return pl.pallas_call(
        functools.partial(mega_kernel, nb),
        out_shape=outs,
        in_specs=[hbm] * 5,
        out_specs=[hbm] * len(outs),
        scratch_shapes=[
            pltpu.VMEM((4, 2, BK, D), BF16), pltpu.VMEM((2, D, D), BF16),
            pltpu.VMEM((2, D, D), F32), pltpu.VMEM((3, 2) + half, F32),
            pltpu.VMEM((2, HALF, D), F32), pltpu.VMEM((8,) + half, F32), pltpu.VMEM((2, 6 * EB, D), F32), pltpu.VMEM((2, EIGHTH, D), F32),
            pltpu.VMEM((PR // 2, PC), F32), pltpu.VMEM((D, D), F32), pltpu.VMEM((HALF, D), F32),
            pltpu.VMEM((HALF, D), F32),
            dma((4, 2)), dma((4, 2)), two, dma((21,)), dma((48,)), dma((48,)), seven, seven,
            many, many, six, six,
        ],
        compiler_params=pltpu.CompilerParams(has_side_effects=True, vmem_limit_bytes=67_043_328),
        name="kfac",
    )(x, dy, w, ainv, sinv)


def finish_kernel(ka, oa, ob, os_, ot, a_old, s_old, a_new, s_new, p, old, new, sem, out_sem):
    scale = (1.0 - FACTOR_DECAY) / (8 * 4096)
    ins = [pltpu.make_async_copy(s, t, sem.at[n]) for n, (s, t) in enumerate(
        ((oa, p.at[0]), (ob, p.at[1]), (a_old, old.at[0]), (os_, p.at[2]), (ot, p.at[3]), (s_old, old.at[1])))]
    outs = [pltpu.make_async_copy(new.at[n], t, out_sem.at[n]) for n, t in enumerate((a_new, s_new))]
    for cp in ins:
        cp.start()

    def blend(n, r, cs, v):
        new[n, r, cs] = FACTOR_DECAY * old[n, r, cs] + scale * v
    c = BLOCKS
    for n in range(2):
        for cp in ins[3 * n:3 * n + 3]:
            cp.wait()
        own, oth = p.at[2 * n], p.at[2 * n + 1]

        @pl.when(ka[0] == 0)
        def _():
            blend(n, c[0], slice(D), own[:, :D])
            blend(n, c[1], c[0], own[:, c[1]].T)
            blend(n, c[1], c[1], own[:, c[4]])
            blend(n, c[1], slice(HALF, D), oth[:, :HALF])

        @pl.when(ka[0] == 1)
        def _():
            blend(n, c[0], c[0], oth[:, c[2]].T)
            blend(n, c[0], c[1], own[:, c[0]].T)
            blend(n, c[0], slice(HALF, D), own[:, HALF:D])
            blend(n, c[1], c[0], oth[:, c[3]].T)
            blend(n, c[1], c[1], own[:, c[1]].T)
            blend(n, c[1], c[2], own[:, c[3]].T)
            blend(n, c[1], c[3], own[:, c[4]])
        outs[n].start()
    for cp in outs:
        cp.wait()


def finish(core, oa, ob, os_, ot, a_old, s_old):
    sd = jax.ShapeDtypeStruct((HALF, D), F32)
    hbm = pl.BlockSpec(memory_space=pltpu.HBM)
    dma = pltpu.SemaphoreType.DMA
    rows = pltpu.VMEM((2, HALF, D), F32)
    return pl.pallas_call(
        finish_kernel,
        out_shape=[sd, sd],
        in_specs=[pl.BlockSpec(memory_space=pltpu.SMEM)] + [hbm] * 6,
        out_specs=[hbm] * 2,
        scratch_shapes=[pltpu.VMEM((4, PR, PC), F32), rows, rows,
                        dma((6,)), dma((2,))],
        compiler_params=pltpu.CompilerParams(vmem_limit_bytes=67_043_328),
        name="blend",
    )(core, oa, ob, os_, ot, a_old, s_old)


def solution(mesh):
    def device_step(x_loc, dy_loc, weights, a_old_rows, s_old_rows, a_inv_rows, s_inv):
        res = mega(x_loc, dy_loc, weights, a_inv_rows, s_inv)
        core = (lax.axis_index("data") % 2).astype(jnp.int32).reshape(1)
        a_new, s_new = finish(core, res[1], res[2], res[3], res[4], a_old_rows, s_old_rows)
        return res[0], a_new, s_new

    row_spec = P("data", None)
    return jax.shard_map(
        device_step,
        mesh=mesh,
        in_specs=(row_spec, row_spec, P(), row_spec, row_spec, row_spec, P()),
        out_specs=(P(), row_spec, row_spec),
        check_vma=False,
    )
```
